32 devices in a mesh: dp: 4 (over y, x), block: 8 (over z, core).
Axes of the slice: x: 2, y: 2, z: 4, core: 2. Of those that a mesh axis runs over, the one named last changes fastest.
Arguments:
- grad_partial: float32 [4, 4, 8, 512, 512], P('dp', None, None, 'block'), may hold values from -6 to 6
- owner_table: int32 [4, 8], replicated, may hold values from 0 to 7, as said below
- left_factor: float32 [4, 8, 2, 512, 512], P('dp', 'block'), as said below
- right_factor: float32 [4, 8, 2, 512, 512], P('dp', 'block'), as said below
Outputs:
- update: bfloat16 [4, 8, 512, 512], P('dp', None, 'block')
- left_out: float32 [4, 8, 2, 512, 512], P('dp', 'block')
- right_out: float32 [4, 8, 2, 512, 512], P('dp', 'block')
The draws below stay inside these ranges and needn't reach their ends.
Inputs may be any that keep to these rules, and one draw needn't show every extreme that they name: owner_table[d, j] is the owner of block (d, j); within each row d no owner appears more than 2 times, and some owner appears exactly 2 times. `left_factor`: each slot holds a symmetric positive definite matrix. `right_factor`: each slot holds a symmetric positive definite matrix.
All inputs are finite; a program needn't handle non-finite values.
Results may differ from the reference program's by a relative error of at most 0.0072.
Values may be sent and summed in bfloat16 or wider, within the bound.
No kernel may reach another device: no remote copies, remote signals or barrier semaphores. Data moves between devices by JAX's collectives and lax.ppermute only.
A program may use at most 128 MiB of HBM per device.

```python
import jax
import jax.numpy as jnp
from jax import lax

P_SIZE = 512
MOST = 2
ITERS = 3
POWER = 8
N_DP = 4
N_BLOCK = 8


def owner_row(row_key):
    first_key, second_key, third_key = jax.random.split(row_key, 3)
    shuffled = jax.random.permutation(first_key, N_BLOCK)
    paired = jax.random.randint(second_key, (), 1, N_BLOCK // 2 + 1)
    position = jnp.arange(N_BLOCK)
    later = jnp.clip(position - paired, 0, N_BLOCK - 1)
    chosen = jnp.where(position < 2 * paired, shuffled[position // 2], shuffled[later])
    return chosen[jax.random.permutation(third_key, N_BLOCK)].astype(jnp.int32)


def draw_owner_table(key, part):
    row_keys = jax.random.split(jax.random.fold_in(key, 11), N_DP)
    return jax.vmap(owner_row)(row_keys)


def factor_draw(key):
    first_key = jax.random.fold_in(key, 0)
    matrix = jax.random.normal(first_key, (N_DP, N_BLOCK, MOST, P_SIZE, P_SIZE), jnp.float32)
    return jnp.einsum('abcij,abckj->abcik', matrix, matrix) / P_SIZE


def draw_left_factor(key, part):
    return factor_draw(jax.random.fold_in(key, 21))


def draw_right_factor(key, part):
    return factor_draw(jax.random.fold_in(key, 31))


def shard_levels(own_key, shape, shards, smallest, largest):
    factor_of, own = 1.0, jax.random.fold_in(own_key, 6)
    for dim, shards_of in shards:
        heights = jnp.exp(jax.random.uniform(jax.random.fold_in(own, dim), (shards_of,), jnp.float32, smallest / len(shards), largest / len(shards)))
        factor_of = factor_of * jnp.repeat(heights, shape[dim] // shards_of).reshape([-1 if axis == dim else 1 for axis in range(len(shape))])
    return factor_of


def bell_draw(rng, dims, spread, reach, pieces=(), kind=jnp.bfloat16):
    level = shard_levels(rng, dims, pieces, -0.22, 0.18) if pieces else 1.0
    drawn = jax.random.normal(rng, dims, jnp.float32) * spread * level
    return jnp.minimum(jnp.maximum(drawn, -reach), reach).astype(kind)


def setup_inputs(seed: int = 0) -> dict:
    key_list = jax.random.split(jax.random.key(seed), 5)
    grad_partial = bell_draw(key_list[0], (N_DP, N_DP, N_BLOCK, P_SIZE, P_SIZE), 1.0, 6.0, ((0, 4), (3, 8)), jnp.float32)
    owner_table = draw_owner_table(jax.random.fold_in(key_list[4], 71), 0)
    left_factor = draw_left_factor(jax.random.fold_in(key_list[4], 71), 0)
    right_factor = draw_right_factor(jax.random.fold_in(key_list[4], 71), 0)
    return dict(grad_partial=grad_partial, owner_table=owner_table, left_factor=left_factor, right_factor=right_factor)


decay_rate = 0.9
damping = 0.1
epsilon = 1e-06

def inverse_root(factor):
    size = factor.shape[0]
    identity = jnp.eye(size, dtype=jnp.float32)
    shifted = factor + damping * identity
    vector = jnp.ones((size,), jnp.float32) / jnp.sqrt(jnp.float32(size))
    length = jnp.float32(1.0)
    for iteration in range(POWER):
        product = jnp.dot(shifted, vector, precision=lax.Precision.HIGHEST)
        length = jnp.sqrt(jnp.sum(product * product))
        vector = product / length
    ceiling = 1.25 * length
    scaled = shifted / ceiling
    inverse = identity * ceiling ** (-0.25)
    for iteration in range(ITERS):
        step_matrix = (5.0 * identity - scaled) / 4.0
        inverse = jnp.dot(inverse, step_matrix, precision=lax.Precision.HIGHEST)
        square = jnp.dot(step_matrix, step_matrix, precision=lax.Precision.HIGHEST)
        fourth = jnp.dot(square, square, precision=lax.Precision.HIGHEST)
        scaled = jnp.dot(fourth, scaled, precision=lax.Precision.HIGHEST)
    return inverse

def precondition(gradient, left_state, right_state):
    size = gradient.shape[0]
    left_term = jnp.dot(gradient, gradient.T, preferred_element_type=jnp.float32) / size
    right_term = jnp.dot(gradient.T, gradient, preferred_element_type=jnp.float32) / size
    new_left = decay_rate * left_state + (1.0 - decay_rate) * left_term
    new_right = decay_rate * right_state + (1.0 - decay_rate) * right_term
    left_root = inverse_root(new_left).astype(jnp.bfloat16)
    right_root = inverse_root(new_right).astype(jnp.bfloat16)
    half = jnp.dot(left_root, gradient, preferred_element_type=jnp.float32).astype(jnp.bfloat16)
    shaped = jnp.dot(half, right_root, preferred_element_type=jnp.float32)
    gradient_wide = gradient.astype(jnp.float32)
    graft_scale = jnp.sqrt(jnp.mean(gradient_wide * gradient_wide)) / jnp.sqrt(jnp.mean(shaped * shaped) + epsilon)
    return ((shaped * graft_scale).astype(jnp.bfloat16), new_left, new_right)

def reference(grad_partial, owner_table, left_factor, right_factor):
    summed = lax.optimization_barrier(jnp.sum(grad_partial, axis=0))
    gradient = summed.astype(jnp.bfloat16).reshape(N_DP * N_BLOCK, P_SIZE, P_SIZE)
    order = jnp.arange(N_BLOCK, dtype=jnp.int32)
    earlier = order[:, None] < order[None, :]
    matching = owner_table[:, :, None] == owner_table[:, None, :]
    slot_rank = lax.optimization_barrier(jnp.sum(jnp.logical_and(matching, earlier[None]), axis=1)).astype(jnp.int32)
    data_index = jnp.repeat(jnp.arange(N_DP, dtype=jnp.int32), N_BLOCK)
    owners = owner_table.reshape(-1).astype(jnp.int32)
    slot_index = slot_rank.reshape(-1)
    left_states = left_factor[data_index, owners, slot_index]
    right_states = right_factor[data_index, owners, slot_index]

    def per_block(block_items):
        return precondition(block_items[0], block_items[1], block_items[2])
    updates, new_lefts, new_rights = lax.map(per_block, (gradient, left_states, right_states))
    left_out = left_factor.at[data_index, owners, slot_index].set(new_lefts)
    right_out = right_factor.at[data_index, owners, slot_index].set(new_rights)
    updates = updates.reshape(N_DP, N_BLOCK, P_SIZE, P_SIZE)
    return (updates, left_out, right_out)
```

```python
import functools

import jax
import jax.numpy as jnp
from jax import lax
from jax.experimental import pallas as pl
from jax.experimental.pallas import tpu as pltpu
from jax.sharding import PartitionSpec as P

MOST = 2
POWER = 8

decay_rate = 0.9
damping = 0.1
epsilon = 1e-06

f32 = jnp.float32
bf16 = jnp.bfloat16
SMEM = pltpu.SMEM
VMEM = pltpu.VMEM
ANY = pl.ANY
LIMIT = 48 * 1024 * 1024


def mm(a, b):
    return jnp.dot(a, b, preferred_element_type=f32)


def arrange_kernel(scal, p_ref, a1_ref, b1_ref, a2_ref, b2_ref, *out_refs):
    count = p_ref.shape[1]
    cut = a2_ref.shape[-1]
    for slot, out_ref in enumerate(out_refs):

        def body(owner, carry, slot=slot, out_ref=out_ref):
            j = scal[3 + slot * count + owner]
            out_ref[owner, :, :cut] = (
                p_ref[0, j, :, :cut] + a1_ref[0, j].astype(f32) + a2_ref[j].astype(f32)
            ).astype(bf16)
            out_ref[owner, :, cut:] = (
                p_ref[0, j, :, cut:] + b1_ref[0, j].astype(f32) + b2_ref[j].astype(f32)
            ).astype(bf16)
            return carry

        lax.fori_loop(0, count, body, 0, unroll=count <= 8)


def arrange(scal, p, a1, b1, a2, b2):
    _, count, stripe, size = p.shape
    cut = size // 2
    out = jax.ShapeDtypeStruct((count, stripe, size), bf16)
    whole = lambda shape: pl.BlockSpec(shape, lambda i, s: (0,) * len(shape))
    return pl.pallas_call(
        arrange_kernel,
        grid_spec=pltpu.PrefetchScalarGridSpec(
            num_scalar_prefetch=1,
            grid=(1,),
            in_specs=[
                pl.BlockSpec((1, count, stripe, size), lambda i, s: (s[0], 0, 0, 0)),
                pl.BlockSpec((1, count, stripe, cut), lambda i, s: (s[1], 0, 0, 0)),
                pl.BlockSpec((1, count, stripe, cut), lambda i, s: (s[2], 0, 0, 0)),
                whole((count, stripe, cut)),
                whole((count, stripe, cut)),
            ],
            out_specs=[whole((count, stripe, size))] * MOST,
        ),
        out_shape=[out] * MOST,
        name="arrange",
    )(scal, p, a1, b1, a2, b2)


def place_kernel(scal, *refs):
    *in_refs, out_ref = refs
    count = out_ref.shape[0]

    def body(j, carry):
        owner = scal[j]
        rank = scal[count + j]
        value = in_refs[0][owner]
        for slot in range(1, MOST):
            value = jnp.where(rank == slot, in_refs[slot][owner], value)
        out_ref[j] = value
        return carry

    lax.fori_loop(0, count, body, 0, unroll=count <= 8)


def place(scal, returned):
    shape = returned[0].shape
    spec = pl.BlockSpec(memory_space=VMEM)
    return pl.pallas_call(
        place_kernel,
        in_specs=[pl.BlockSpec(memory_space=SMEM)] + [spec] * MOST,
        out_specs=spec,
        out_shape=jax.ShapeDtypeStruct(shape, bf16),
        name="place",
    )(scal, *returned)


def add_diagonal(ref, k, value):
    size = ref.shape[1]
    width = min(size, 128)
    rows = lax.broadcasted_iota(jnp.int32, (width, width), 0)
    columns = lax.broadcasted_iota(jnp.int32, (width, width), 1)
    spread = jnp.where(rows == columns, value, 0.0)
    for start in range(0, size, width):
        part = pl.ds(start, width)
        ref[k, part, part] += spread


def slot_kernel(slot, chained, active_ref, g_ref, l_hbm, r_hbm, *refs):
    refs = refs[2 * chained :]
    u_ref, lo_hbm, ro_hbm = refs[:3]
    s_ref, n_ref, *wides, y_ref, mb_narrow, tb_narrow, ub_ref, yb_ref, in_sem, out_sem = refs[3:]
    size = g_ref.shape[0]
    sides = (0, 1)
    states = (l_hbm, r_hbm)
    news = (lo_hbm, ro_hbm)
    loads = [pltpu.make_async_copy(states[k].at[slot], s_ref.at[k], in_sem.at[k]) for k in sides]
    stores = [pltpu.make_async_copy(n_ref.at[k], news[k].at[slot], out_sem.at[k]) for k in sides]
    for k in sides:
        loads[k].start()
    active = active_ref[slot] > 0

    @pl.when(active)
    def _():
        m_ref, t_ref = wides
        mb_ref, tb_ref = mb_narrow, tb_narrow
        g = g_ref[...]
        contract = ((1,), (0,))
        for k in sides:
            dims = ((contract[k], contract[k]), ((), ()))
            term = lax.dot_general(g, g, dims, preferred_element_type=f32)
            loads[k].wait()
            new = decay_rate * s_ref[k] + term * ((1.0 - decay_rate) / size)
            n_ref[k] = new
            m_ref[k] = new
            stores[k].start()
        for k in sides:
            add_diagonal(m_ref, k, jnp.full((1, 1), damping, f32))

        vectors = [jnp.full((1, size), size**-0.5, f32)] * 2
        lengths = [None, None]
        for turn in range(POWER):
            for k in sides:
                vectors[k] = jnp.sum(m_ref[k] * vectors[k], axis=1 - turn % 2, keepdims=True)
            for k in sides:
                square = jnp.sum(vectors[k] * vectors[k], axis=turn % 2, keepdims=True)
                lengths[k] = jnp.sqrt(square)
                vectors[k] = vectors[k] / lengths[k]

        scales = []
        for k in sides:
            ceiling = 1.25 * lengths[k]
            scales.append(lax.rsqrt(jnp.sqrt(ceiling)))
            scaled = m_ref[k] * (1.0 / ceiling)
            m_ref[k] = scaled
            mb_ref[k] = scaled.astype(bf16)
        for step in range(2):
            for k in sides:
                t = mm(mb_ref[k], mb_ref[k]) * (1 / 16) - 0.625 * m_ref[k]
                t_ref[k] = t
                tb_ref[k] = t.astype(bf16)
            for k in sides:
                ub_ref[k] = (3.125 * t_ref[k] + mm(tb_ref[k], tb_ref[k])).astype(bf16)
            for k in sides:
                t = (625 / 256) * m_ref[k] + mm(ub_ref[k], mb_ref[k])
                t_ref[k] = t
                tb_ref[k] = t.astype(bf16)
            if step == 0:
                for k in sides:
                    y = mm(mb_ref[k], tb_ref[k]) * (1 / 16) - 0.3125 * (m_ref[k] + t_ref[k])
                    y_ref[k] = y
                    yb_ref[k] = y.astype(bf16)
                m_ref, t_ref = t_ref, m_ref
                mb_ref, tb_ref = tb_ref, mb_ref
        for k in sides:
            x = 1.25 * y_ref[k] - (25 / 64) * t_ref[k] - 0.25 * mm(yb_ref[k], tb_ref[k])
            m_ref[k] = x * scales[k]
            add_diagonal(m_ref, k, (125 / 64) * scales[k])
            mb_ref[k] = m_ref[k].astype(bf16)

        mb_ref[0] = mm(mb_ref[0], g).astype(bf16)
        shaped = mm(mb_ref[0], mb_ref[1])
        m_ref[0] = shaped
        wide = g.astype(f32)
        count = size * size
        top = jnp.sum(jnp.sum(wide * wide, axis=0, keepdims=True), axis=1, keepdims=True) / count
        bottom = jnp.sum(jnp.sum(shaped * shaped, axis=0, keepdims=True), axis=1, keepdims=True) / count
        u_ref[...] = (m_ref[0] * (jnp.sqrt(top) / jnp.sqrt(bottom + epsilon))).astype(bf16)

    @pl.when(jnp.logical_not(active))
    def _():
        for k in sides:
            loads[k].wait()
            n_ref[k] = s_ref[k]
            stores[k].start()
        u_ref[...] = jnp.zeros_like(u_ref)

    for k in sides:
        stores[k].wait()


def run_slot(slot, active, g, left, right, chain):
    size = g.shape[-1]
    any_spec = pl.BlockSpec(memory_space=ANY)
    vmem_spec = pl.BlockSpec(memory_space=VMEM)
    wide = pltpu.VMEM((2, size, size), f32)
    narrow = pltpu.VMEM((2, size, size), bf16)
    chained = len(chain) // 2
    return pl.pallas_call(
        functools.partial(slot_kernel, slot, chained),
        in_specs=[pl.BlockSpec(memory_space=SMEM), vmem_spec, any_spec, any_spec]
        + [any_spec] * len(chain),
        out_specs=[vmem_spec, any_spec, any_spec],
        out_shape=[
            jax.ShapeDtypeStruct((size, size), bf16),
            jax.ShapeDtypeStruct(left.shape, f32),
            jax.ShapeDtypeStruct(right.shape, f32),
        ],
        scratch_shapes=[wide] * 5
        + [narrow] * 4
        + [pltpu.SemaphoreType.DMA((2,)), pltpu.SemaphoreType.DMA((2,))],
        input_output_aliases={4: 1, 5: 2} if chained else {},
        compiler_params=pltpu.CompilerParams(vmem_limit_bytes=LIMIT),
        cost_estimate=pl.CostEstimate(
            flops=40 * size**3, bytes_accessed=18 * size**2, transcendentals=0
        ),
        name=f"slot{slot}",
    )(active, g, left, right, *chain)


def tables(table_row, owner_index, count):
    order = jnp.arange(count, dtype=jnp.int32)
    earlier = order[:, None] < order[None, :]
    matching = table_row[:, None] == table_row[None, :]
    rank = jnp.sum(jnp.logical_and(matching, earlier), axis=0).astype(jnp.int32)
    slots = jnp.arange(MOST, dtype=jnp.int32)
    chooser = jnp.logical_and(
        table_row[None, None, :] == order[None, :, None],
        rank[None, None, :] == slots[:, None, None],
    )
    block_of = jnp.sum(jnp.where(chooser, order, 0), axis=2).astype(jnp.int32)
    mine = jnp.logical_and(table_row[None, :] == owner_index, rank[None, :] == slots[:, None])
    active = jnp.sum(mine, axis=1).astype(jnp.int32)
    return block_of.reshape(-1), rank, active


def local(grad_partial, owner_table, left_factor, right_factor):
    p = grad_partial[0]
    rows, count, stripe, size = p.shape
    data_index = lax.axis_index("dp")
    owner_index = lax.axis_index("block")
    table_row = lax.dynamic_index_in_dim(owner_table, data_index, 0, keepdims=False)
    block_of, rank, active = tables(table_row, owner_index, count)

    low, high = data_index % 2, data_index // 2
    cut = size // 2
    half_a = p[..., :cut].reshape(2, 2, count, stripe, cut)
    half_b = p[..., cut:].reshape(2, 2, count, stripe, cut)
    over_low = [(i, i ^ 1) for i in range(rows)]
    over_high = [(i, i ^ 2) for i in range(rows)]
    pick = functools.partial(lax.dynamic_index_in_dim, keepdims=False)
    a1 = lax.ppermute(pick(half_a, 1 - low, 1).astype(bf16), "dp", over_low)
    b1 = lax.ppermute(pick(half_b, 1 - high, 0).astype(bf16), "dp", over_high)
    a2 = pick(pick(half_a, 1 - high, 0), low, 0) + pick(a1, 1 - high, 0).astype(f32)
    a2 = lax.ppermute(a2.astype(bf16), "dp", over_high)
    b2 = pick(pick(half_b, high, 0), 1 - low, 0) + pick(b1, 1 - low, 0).astype(f32)
    b2 = lax.ppermute(b2.astype(bf16), "dp", over_low)
    scal = jnp.concatenate([jnp.stack([data_index, high, low]).astype(jnp.int32), block_of])
    outgoing = arrange(scal, p, a1, b1, a2, b2)

    left, right = left_factor[0, 0], right_factor[0, 0]
    received = [lax.all_to_all(out, "block", 0, 0, tiled=True) for out in outgoing]
    chain = ()
    returned = []
    for slot in range(MOST):
        update, *chain = run_slot(
            slot, active, received[slot].reshape(size, size), left, right, tuple(chain)
        )
        returned.append(
            lax.all_to_all(update.reshape(count, stripe, size), "block", 0, 0, tiled=True)
        )
    placed = place(jnp.concatenate([table_row, rank]), returned)
    new_left, new_right = chain
    return placed[None], new_left[None, None], new_right[None, None]


def solution(mesh):
    placed = (
        P("dp", None, None, "block", None),
        P(),
        P("dp", "block", None, None, None),
        P("dp", "block", None, None, None),
    )
    return jax.shard_map(
        local,
        mesh=mesh,
        in_specs=placed,
        out_specs=(
            P("dp", None, "block", None),
            P("dp", "block", None, None, None),
            P("dp", "block", None, None, None),
        ),
        check_vma=False,
    )
```

```python
import functools

import jax
import jax.numpy as jnp
from jax import lax
from jax.experimental import pallas as pl
from jax.experimental.pallas import tpu as pltpu
from jax.sharding import PartitionSpec as P


MOST = 2
POWER = 8

decay_rate = 0.9
damping = 0.1
epsilon = 1e-06

f32 = jnp.float32
bf16 = jnp.bfloat16
SMEM = pltpu.SMEM
VMEM = pltpu.VMEM
ANY = pltpu.HBM
LIMIT = 24 * 1024 * 1024
SMALL = 8 * 1024 * 1024


def mm(a, b):
    return jnp.dot(a, b, preferred_element_type=f32)


def call(kernel, out_shape, scratch, operands, flops=0, aliases={}, limit=SMALL):
    outs = [shape for shape, _ in out_shape]
    size = sum(array.size * array.dtype.itemsize for array, _ in operands)
    return pl.pallas_call(
        kernel,
        in_specs=[pl.BlockSpec(memory_space=space) for _, space in operands],
        out_specs=[pl.BlockSpec(memory_space=space) for _, space in out_shape],
        out_shape=outs,
        scratch_shapes=scratch,
        input_output_aliases=aliases,
        compiler_params=pltpu.CompilerParams(vmem_limit_bytes=limit),
        cost_estimate=pl.CostEstimate(flops=flops, bytes_accessed=size, transcendentals=0),
    )(*[array for array, _ in operands])


def cast_kernel(scal, p_ref, a_ref, b_ref):
    cut = a_ref.shape[-1]
    high, low = scal[0], scal[1]
    for other in range(2):
        a_ref[other] = p_ref[other, 1 - low, :, :, :cut].astype(bf16)
        b_ref[other] = p_ref[1 - high, other, :, :, cut:].astype(bf16)


def keep_kernel(scal, p_ref, a_ref, b_ref):
    cut = a_ref.shape[-1]
    high, low = scal[0], scal[1]
    a_ref[...] = p_ref[1 - high, low, :, :, :cut]
    b_ref[...] = p_ref[high, 1 - low, :, :, cut:]


def half_kernel(scal, p_ref, a1_ref, b1_ref, own_ref):
    cut = a1_ref.shape[-1]
    high, low = scal[0], scal[1]
    own_ref[:, :, :cut] = p_ref[high, low, :, :, :cut] + a1_ref[high].astype(f32)
    own_ref[:, :, cut:] = p_ref[high, low, :, :, cut:] + b1_ref[low].astype(f32)


def forward_kernel(scal, pa_ref, pb_ref, a1_ref, b1_ref, a_ref, b_ref):
    high, low = scal[0], scal[1]
    a_ref[...] = (pa_ref[...] + a1_ref[1 - high].astype(f32)).astype(bf16)
    b_ref[...] = (pb_ref[...] + b1_ref[1 - low].astype(f32)).astype(bf16)


def total_kernel(own_ref, a2_ref, b2_ref, out_ref):
    cut = a2_ref.shape[-1]
    out_ref[:, :, :cut] = (own_ref[:, :, :cut] + a2_ref[...].astype(f32)).astype(bf16)
    out_ref[:, :, cut:] = (own_ref[:, :, cut:] + b2_ref[...].astype(f32)).astype(bf16)


def sum_over_dp(grad_partial, scal):
    rows, count, stripe, size = grad_partial.shape
    p = grad_partial.reshape(2, rows // 2, count, stripe, size)
    over_low = [(i, i ^ 1) for i in range(rows)]
    over_high = [(i, i ^ 2) for i in range(rows)]
    shape = (count, stripe, size // 2)
    pair = (jax.ShapeDtypeStruct((2,) + shape, bf16), VMEM)
    one = (jax.ShapeDtypeStruct(shape, bf16), VMEM)
    both = (jax.ShapeDtypeStruct((count, stripe, size), bf16), VMEM)
    fixed = [(scal, SMEM), (p, VMEM)]
    a, b = call(cast_kernel, [pair] * 2, [], fixed)
    first = [lax.ppermute(a, "dp", over_low), lax.ppermute(b, "dp", over_high)]
    kept = [(jax.ShapeDtypeStruct(shape, f32), VMEM)] * 2
    pa, pb = call(keep_kernel, kept, [], fixed)
    arrived = [(array, VMEM) for array in first]
    operands = [(scal, SMEM), (pa, VMEM), (pb, VMEM)] + arrived
    a, b = call(forward_kernel, [one] * 2, [], operands)
    second = [lax.ppermute(a, "dp", over_high), lax.ppermute(b, "dp", over_low)]
    whole = [(jax.ShapeDtypeStruct((count, stripe, size), f32), VMEM)]
    (own,) = call(half_kernel, whole, [], fixed + arrived)
    operands = [(own, VMEM)] + [(array, VMEM) for array in second]
    (total,) = call(total_kernel, [both], [], operands)
    return total


def arrange_kernel(count, scal, own_ref, other_ref, *out_refs):
    me = scal[2]
    core, chip = me % 2, me // 2
    chips = count // 2
    for slot in range(MOST):
        for r in range(chips):
            j = scal[3 + slot * count + lax.bitwise_xor(chip, r) * 2 + core]
            out_ref = out_refs[slot * chips + r]
            out_ref[core] = own_ref[j]
            out_ref[1 - core] = other_ref[j]


def stage_kernel(l_ref, r_ref, l_out, r_out):
    l_out[...] = l_ref[...]
    r_out[...] = r_ref[...]


def give_kernel(scal, *refs):
    *in_refs, out_ref = refs
    core = scal[2] % 2
    for r, in_ref in enumerate(in_refs):
        out_ref[r] = in_ref[1 - core]


def place_kernel(count, scal, *refs):
    *in_refs, out_ref = refs
    me = scal[2]
    core, chip = me % 2, me // 2
    chips = count // 2
    pieces = []
    for r in range(chips):
        base = lax.bitwise_xor(chip, r) * 2
        pieces.append((base + core, in_refs[r], core))
        pieces.append((base + 1 - core, in_refs[chips], r))
    for q in range(count):
        pieces.append((count + lax.bitwise_xor(me, q), in_refs[chips + 1 + q], None))
    for entry, ref, index in pieces:
        at = 3 + entry

        @pl.when(scal[at + MOST * count] > 0)
        def _(at=at, ref=ref, index=index):
            out_ref[scal[at]] = ref[...] if index is None else ref[index]


def over_block(arrays, count, stride):
    return [arrays[0]] + [
        lax.ppermute(array, "block", [(i, i ^ (r * stride)) for i in range(count)])
        for r, array in enumerate(arrays)
        if r > 0
    ]


def add_diagonal(ref, k, value):
    size = ref.shape[1]
    width = min(size, 128)
    rows = lax.broadcasted_iota(jnp.int32, (width, width), 0)
    columns = lax.broadcasted_iota(jnp.int32, (width, width), 1)
    spread = jnp.where(rows == columns, value, 0.0)
    for start in range(0, size, width):
        part = pl.ds(start, width)
        ref[k, part, part] += spread


def slot_kernel(slot, direct, count, scal, l_ref, r_ref, *refs):
    chips = count // 2
    in_refs, refs = refs[:chips], refs[chips + (2 if slot else 0) :]
    n_out = count if direct else chips
    out_refs, refs = refs[:n_out], refs[n_out:]
    lo_hbm, ro_hbm, g_ref, n_ref, *wides, y_ref = refs[:7]
    mb_narrow, tb_narrow, ub_ref, yb_ref, out_sem = refs[7:]
    size = g_ref.shape[0]
    stripe = size // count
    me = scal[2]
    chip = me // 2
    sides = (0, 1)
    states = (l_ref, r_ref)
    news = (lo_hbm, ro_hbm)
    stores = [pltpu.make_async_copy(n_ref.at[k], news[k].at[slot], out_sem.at[k]) for k in sides]
    active = scal[3 + (MOST + slot) * count + me] > 0

    @pl.when(active)
    def _():
        m_ref, t_ref = wides
        mb_ref, tb_ref = mb_narrow, tb_narrow
        for r, ref in enumerate(in_refs):
            for c in range(2):
                start = pl.multiple_of((lax.bitwise_xor(chip, r) * 2 + c) * stripe, stripe)
                g_ref[pl.ds(start, stripe), :] = ref[c]
        g = g_ref[...]
        contract = ((1,), (0,))
        for k in sides:
            dims = ((contract[k], contract[k]), ((), ()))
            term = lax.dot_general(g, g, dims, preferred_element_type=f32)
            new = decay_rate * states[k][slot] + term * ((1.0 - decay_rate) / size)
            n_ref[k] = new
            m_ref[k] = new
            stores[k].start()
        for k in sides:
            add_diagonal(m_ref, k, jnp.full((1, 1), damping, f32))

        vectors = [jnp.full((1, size), size**-0.5, f32)] * 2
        lengths = [None, None]
        for turn in range(POWER):
            for k in sides:
                vectors[k] = jnp.sum(m_ref[k] * vectors[k], axis=1 - turn % 2, keepdims=True)
            for k in sides:
                square = jnp.sum(vectors[k] * vectors[k], axis=turn % 2, keepdims=True)
                lengths[k] = jnp.sqrt(square)
                vectors[k] = vectors[k] / lengths[k]

        scales = []
        for k in sides:
            ceiling = 1.25 * lengths[k]
            scales.append(lax.rsqrt(jnp.sqrt(ceiling)))
            scaled = m_ref[k] * (1.0 / ceiling)
            m_ref[k] = scaled
            mb_ref[k] = scaled.astype(bf16)
        for step in range(2):
            for k in sides:
                t = mm(mb_ref[k], mb_ref[k]) * (1 / 16) - 0.625 * m_ref[k]
                t_ref[k] = t
                tb_ref[k] = t.astype(bf16)
            for k in sides:
                ub_ref[k] = (3.125 * t_ref[k] + mm(tb_ref[k], tb_ref[k])).astype(bf16)
            for k in sides:
                t = (625 / 256) * m_ref[k] + mm(ub_ref[k], mb_ref[k])
                t_ref[k] = t
                tb_ref[k] = t.astype(bf16)
            if step == 0:
                for k in sides:
                    y = mm(mb_ref[k], tb_ref[k]) * (1 / 16) - 0.3125 * (m_ref[k] + t_ref[k])
                    y_ref[k] = y
                    yb_ref[k] = y.astype(bf16)
                m_ref, t_ref = t_ref, m_ref
                mb_ref, tb_ref = tb_ref, mb_ref
        for k in sides:
            x = 1.25 * y_ref[k] - (25 / 64) * t_ref[k] - 0.25 * mm(yb_ref[k], tb_ref[k])
            m_ref[k] = x * scales[k]
            add_diagonal(m_ref, k, (125 / 64) * scales[k])
            mb_ref[k] = m_ref[k].astype(bf16)

        mb_ref[0] = mm(mb_ref[0], g).astype(bf16)
        shaped = mm(mb_ref[0], mb_ref[1])
        m_ref[0] = shaped
        wide = g.astype(f32)
        entries = size * size
        top = jnp.sum(jnp.sum(wide * wide, axis=0, keepdims=True), axis=1, keepdims=True) / entries
        bottom = jnp.sum(jnp.sum(shaped * shaped, axis=0, keepdims=True), axis=1, keepdims=True) / entries
        scale = jnp.sqrt(top) / jnp.sqrt(bottom + epsilon)

        def rows_of(device):
            part = pl.ds(pl.multiple_of(device * stripe, stripe), stripe)
            return (m_ref[0, part, :] * scale).astype(bf16)

        if direct:
            for q in range(count):
                out_refs[q][...] = rows_of(lax.bitwise_xor(me, q))
        else:
            for r in range(chips):
                for c in range(2):
                    out_refs[r][c] = rows_of(lax.bitwise_xor(chip, r) * 2 + c)

    @pl.when(jnp.logical_not(active))
    def _():
        for k in sides:
            n_ref[k] = states[k][slot]
            stores[k].start()
        for out_ref in out_refs:
            out_ref[...] = jnp.zeros_like(out_ref)

    for k in sides:
        stores[k].wait()


def run_slot(slot, direct, scal, pieces, left, right, chain):
    size = left.shape[-1]
    stripe = pieces[0].shape[1]
    count = size // stripe
    wide = pltpu.VMEM((2, size, size), f32)
    narrow = pltpu.VMEM((2, size, size), bf16)
    sem = pltpu.SemaphoreType.DMA((2,))
    if direct:
        out = [(jax.ShapeDtypeStruct((stripe, size), bf16), VMEM)] * count
    else:
        out = [(jax.ShapeDtypeStruct((2, stripe, size), bf16), VMEM)] * (count // 2)
    news = [(jax.ShapeDtypeStruct(state.shape, f32), ANY) for state in (left, right)]
    operands = [(scal, SMEM), (left, VMEM), (right, VMEM)] + [(piece, VMEM) for piece in pieces]
    operands += [(state, ANY) for state in chain]
    aliases = {len(operands) - 2 + k: len(out) + k for k in range(2)} if chain else {}
    *updates, new_left, new_right = call(
        functools.partial(slot_kernel, slot, direct, count),
        out + news,
        [pltpu.VMEM((size, size), bf16)] + [wide] * 4 + [narrow] * 4 + [sem],
        operands,
        flops=40 * size**3,
        aliases=aliases,
        limit=LIMIT,
    )
    return updates, (new_left, new_right)


def tables(table_row, count):
    order = jnp.arange(count, dtype=jnp.int32)
    earlier = order[:, None] < order[None, :]
    matching = table_row[:, None] == table_row[None, :]
    rank = jnp.sum(jnp.logical_and(matching, earlier), axis=0).astype(jnp.int32)
    slots = jnp.arange(MOST, dtype=jnp.int32)
    chooser = jnp.logical_and(
        table_row[None, None, :] == order[None, :, None],
        rank[None, None, :] == slots[:, None, None],
    )
    block_of = jnp.sum(jnp.where(chooser, order, 0), axis=2).astype(jnp.int32)
    used = jnp.sum(chooser, axis=2).astype(jnp.int32)
    return jnp.concatenate([block_of.reshape(-1), used.reshape(-1)])


def step(grad_partial, owner_table, left_factor, right_factor):
    _, count, stripe, size = grad_partial.shape[1:]
    data_index = lax.axis_index("dp").astype(jnp.int32)
    owner_index = lax.axis_index("block").astype(jnp.int32)
    table_row = lax.dynamic_index_in_dim(owner_table, data_index, 0, keepdims=False)
    place_of = jnp.stack([data_index // 2, data_index % 2, owner_index])
    scal = jnp.concatenate([place_of, tables(table_row, count)])
    left, right = left_factor[0, 0], right_factor[0, 0]

    chips = count // 2
    cores = [(i, i ^ 1) for i in range(count)]
    total = sum_over_dp(grad_partial[0], place_of)
    other = lax.ppermute(total, "block", cores)
    message = (jax.ShapeDtypeStruct((2, stripe, size), bf16), VMEM)
    messages = call(
        functools.partial(arrange_kernel, count),
        [message] * (MOST * chips),
        [],
        [(scal, SMEM), (total, VMEM), (other, VMEM)],
    )
    pieces = []
    for slot in range(MOST):
        pieces.append(over_block(messages[slot * chips : (slot + 1) * chips], count, 2))

    states = [(state, VMEM) for state in (left, right)]
    kept = [(jax.ShapeDtypeStruct(left.shape, f32), VMEM)] * 2
    left, right = call(stage_kernel, kept, [], states)

    updates, chain = run_slot(0, False, scal, pieces[0], left, right, ())
    returned = over_block(updates, count, 2)
    updates, chain = run_slot(1, True, scal, pieces[1], left, right, chain)
    direct = over_block(updates, count, 1)
    (given,) = call(
        give_kernel,
        [(jax.ShapeDtypeStruct((chips, stripe, size), bf16), VMEM)],
        [],
        [(scal, SMEM)] + [(piece, VMEM) for piece in returned],
    )
    given = lax.ppermute(given, "block", cores)
    (placed,) = call(
        functools.partial(place_kernel, count),
        [(jax.ShapeDtypeStruct((count, stripe, size), bf16), VMEM)],
        [],
        [(scal, SMEM)] + [(piece, VMEM) for piece in returned + [given] + direct],
    )
    new_left, new_right = chain
    return placed[None], new_left[None, None], new_right[None, None]


def solution(mesh):
    placed = (
        P("dp", None, None, "block", None),
        P(),
        P("dp", "block", None, None, None),
        P("dp", "block", None, None, None),
    )
    return jax.shard_map(
        step,
        mesh=mesh,
        in_specs=placed,
        out_specs=(
            P("dp", None, "block", None),
            P("dp", "block", None, None, None),
            P("dp", "block", None, None, None),
        ),
        check_vma=False,
    )
```

```python
import functools

import jax
import jax.numpy as jnp
from jax import lax
from jax.experimental import pallas as pl
from jax.experimental.pallas import tpu as pltpu
from jax.sharding import PartitionSpec as P


MOST = 2
POWER = 8
CENTER = 3.6

decay_rate = 0.9
damping = 0.1
epsilon = 1e-06

f32 = jnp.float32
bf16 = jnp.bfloat16
SMEM = pltpu.SMEM
VMEM = pltpu.VMEM
ANY = pltpu.HBM
LIMIT = 24 * 1024 * 1024
SMALL = 8 * 1024 * 1024


def mm(a, b):
    return jnp.dot(a, b, preferred_element_type=f32)


def call(kernel, out_shape, scratch, operands, flops=0, aliases={}, limit=SMALL):
    outs = [shape for shape, _ in out_shape]
    size = sum(array.size * array.dtype.itemsize for array, _ in operands)
    return pl.pallas_call(
        kernel,
        in_specs=[pl.BlockSpec(memory_space=space) for _, space in operands],
        out_specs=[pl.BlockSpec(memory_space=space) for _, space in out_shape],
        out_shape=outs,
        scratch_shapes=scratch,
        input_output_aliases=aliases,
        compiler_params=pltpu.CompilerParams(vmem_limit_bytes=limit),
        cost_estimate=pl.CostEstimate(flops=flops, bytes_accessed=size, transcendentals=0),
    )(*[array for array, _ in operands])


def cast_kernel(scal, p_ref, a_ref, b_ref):
    cut = a_ref.shape[-1]
    high, low = scal[0], scal[1]
    for other in range(2):
        a_ref[other] = p_ref[other, 1 - low, :, :, :cut].astype(bf16)
        b_ref[other] = p_ref[1 - high, other, :, :, cut:].astype(bf16)


def keep_kernel(scal, p_ref, a_ref, b_ref):
    cut = a_ref.shape[-1]
    high, low = scal[0], scal[1]
    a_ref[...] = p_ref[1 - high, low, :, :, :cut]
    b_ref[...] = p_ref[high, 1 - low, :, :, cut:]


def half_kernel(scal, p_ref, a1_ref, b1_ref, own_ref):
    cut = a1_ref.shape[-1]
    high, low = scal[0], scal[1]
    own_ref[:, :, :cut] = p_ref[high, low, :, :, :cut] + a1_ref[high].astype(f32)
    own_ref[:, :, cut:] = p_ref[high, low, :, :, cut:] + b1_ref[low].astype(f32)


def forward_kernel(bit, scal, kept_ref, first_ref, out_ref):
    out_ref[...] = (kept_ref[...] + first_ref[1 - scal[bit]].astype(f32)).astype(bf16)


def total_kernel(own_ref, a2_ref, b2_ref, out_ref):
    cut = a2_ref.shape[-1]
    out_ref[:, :, :cut] = (own_ref[:, :, :cut] + a2_ref[...].astype(f32)).astype(bf16)
    out_ref[:, :, cut:] = (own_ref[:, :, cut:] + b2_ref[...].astype(f32)).astype(bf16)


def sum_over_dp(grad_partial, scal):
    rows, count, stripe, size = grad_partial.shape
    p = grad_partial.reshape(2, rows // 2, count, stripe, size)
    over_low = [(i, i ^ 1) for i in range(rows)]
    over_high = [(i, i ^ 2) for i in range(rows)]
    shape = (count, stripe, size // 2)
    pair = (jax.ShapeDtypeStruct((2,) + shape, bf16), VMEM)
    one = (jax.ShapeDtypeStruct(shape, bf16), VMEM)
    both = (jax.ShapeDtypeStruct((count, stripe, size), bf16), VMEM)
    fixed = [(scal, SMEM), (p, VMEM)]
    a, b = call(cast_kernel, [pair] * 2, [], fixed)
    first = [lax.ppermute(a, "dp", over_low), lax.ppermute(b, "dp", over_high)]
    kept = [(jax.ShapeDtypeStruct(shape, f32), VMEM)] * 2
    pa, pb = call(keep_kernel, kept, [], fixed)
    arrived = [(array, VMEM) for array in first]
    second = []
    for bit, (kept, perm) in enumerate([(pa, over_high), (pb, over_low)]):
        operands = [(scal, SMEM), (kept, VMEM), (first[bit], VMEM)]
        (summed,) = call(functools.partial(forward_kernel, bit), [one], [], operands)
        second.append(lax.ppermute(summed, "dp", perm))
    whole = [(jax.ShapeDtypeStruct((count, stripe, size), f32), VMEM)]
    (own,) = call(half_kernel, whole, [], fixed + arrived)
    operands = [(own, VMEM)] + [(array, VMEM) for array in second]
    (total,) = call(total_kernel, [both], [], operands)
    return total


def arrange_kernel(count, scal, own_ref, other_ref, *out_refs):
    me = scal[2]
    core, chip = me % 2, me // 2
    chips = count // 2
    for slot in range(MOST):
        for r in range(chips):
            j = scal[3 + slot * count + lax.bitwise_xor(chip, r) * 2 + core]
            out_ref = out_refs[slot * chips + r]
            out_ref[core] = own_ref[j]
            out_ref[1 - core] = other_ref[j]


def stage_kernel(l_ref, r_ref, l_out, r_out):
    l_out[...] = l_ref[...]
    r_out[...] = r_ref[...]


def give_kernel(scal, *refs):
    *in_refs, out_ref = refs
    core = scal[2] % 2
    for r, in_ref in enumerate(in_refs):
        out_ref[r] = in_ref[1 - core]


def place_kernel(count, scal, *refs):
    *in_refs, out_ref = refs
    me = scal[2]
    core, chip = me % 2, me // 2
    chips = count // 2
    pieces = []
    for r in range(chips):
        base = lax.bitwise_xor(chip, r) * 2
        pieces.append((base + core, in_refs[r], core))
        pieces.append((base + 1 - core, in_refs[chips], r))
    for q in range(count):
        pieces.append((count + lax.bitwise_xor(me, q), in_refs[chips + 1 + q], None))
    for entry, ref, index in pieces:
        at = 3 + entry

        @pl.when(scal[at + MOST * count] > 0)
        def _(at=at, ref=ref, index=index):
            out_ref[scal[at]] = ref[...] if index is None else ref[index]


def over_block(arrays, count, stride):
    moved = [arrays[0]]
    for r in range(1, len(arrays)):
        pairs = [(i, i ^ (r * stride)) for i in range(count)]
        moved.append(lax.ppermute(arrays[r], "block", pairs))
    return moved


def add_diagonal(ref, k, value):
    size = ref.shape[1]
    width = min(size, 128)
    rows = lax.broadcasted_iota(jnp.int32, (width, width), 0)
    columns = lax.broadcasted_iota(jnp.int32, (width, width), 1)
    spread = jnp.where(rows == columns, value, 0.0)
    for start in range(0, size, width):
        part = pl.ds(start, width)
        ref[k, part, part] += spread


def times_row(ref, k, row):
    size = ref.shape[1]
    step = min(size, 64)
    return jnp.concatenate(
        [
            jnp.sum(ref[k, pl.ds(start, step), :] * row, axis=1, keepdims=True)
            for start in range(0, size, step)
        ]
    )


def times_column(ref, k, column):
    total = 0.0
    for start in range(0, ref.shape[1], 8):
        total += ref[k, pl.ds(start, 8), :] * column[start : start + 8]
    return jnp.sum(total, axis=0, keepdims=True)


def product(a_ref, b_ref, k):
    half = a_ref.shape[1] // 2
    return mm(a_ref[k, :half, :], b_ref[k]), mm(a_ref[k, half:, :], b_ref[k, :, half:])


def upper(ref, k):
    half = ref.shape[1] // 2
    return ref[k, :half, :], ref[k, half:, half:]


def store(ref, k, blocks):
    half = ref.shape[1] // 2
    ref[k, :half, :] = blocks[0]
    ref[k, half:, half:] = blocks[1]


def mirror(ref, k, blocks):
    half = ref.shape[1] // 2
    top = blocks[0].astype(bf16)
    ref[k, :half, :] = top
    ref[k, half:, half:] = blocks[1].astype(bf16)
    ref[k, half:, :half] = top[:, half:].T


def slot_kernel(slot, direct, count, scal, l_ref, r_ref, *refs):
    chips = count // 2
    in_refs, refs = refs[:chips], refs[chips + (2 if slot else 0) :]
    n_out = count if direct else chips
    out_refs, refs = refs[:n_out], refs[n_out:]
    lo_hbm, ro_hbm, g_ref, n_ref, m_ref, t_ref, y_ref, w_ref = refs[:8]
    mb_ref, tb_ref, ub_ref, vb_ref, out_sem = refs[8:]
    size = g_ref.shape[0]
    stripe = size // count
    me = scal[2]
    chip = me // 2
    sides = (0, 1)
    states = (l_ref, r_ref)
    news = (lo_hbm, ro_hbm)
    stores = [pltpu.make_async_copy(n_ref.at[k], news[k].at[slot], out_sem.at[k]) for k in sides]
    active = scal[3 + (MOST + slot) * count + me] > 0

    @pl.when(active)
    def _():
        for r, ref in enumerate(in_refs):
            for c in range(2):
                start = pl.multiple_of((lax.bitwise_xor(chip, r) * 2 + c) * stripe, stripe)
                g_ref[pl.ds(start, stripe), :] = ref[c]
        g = g_ref[...]
        contract = ((1,), (0,))
        for k in sides:
            dims = ((contract[k], contract[k]), ((), ()))
            term = lax.dot_general(g, g, dims, preferred_element_type=f32)
            new = decay_rate * states[k][slot] + term * ((1.0 - decay_rate) / size)
            n_ref[k] = new
            m_ref[k] = new
            stores[k].start()
        for k in sides:
            add_diagonal(m_ref, k, jnp.full((1, 1), damping, f32))

        vectors = [jnp.full((1, size), size**-0.5, f32)] * 2
        lengths = [None, None]
        for turn in range(POWER):
            for k in sides:
                vectors[k] = (times_column if turn % 2 else times_row)(m_ref, k, vectors[k])
            for k in sides:
                square = jnp.sum(vectors[k] * vectors[k], axis=turn % 2, keepdims=True)
                lengths[k] = jnp.sqrt(square)
                vectors[k] = vectors[k] / lengths[k]

        scales = []
        for k in sides:
            ceiling = 1.25 * lengths[k]
            scales.append(lax.rsqrt(jnp.sqrt(ceiling)))
            scaled = m_ref[k] * (1.0 / ceiling)
            m_ref[k] = scaled
            mb_ref[k] = scaled.astype(bf16)
        for k in sides:
            t = [p * (1 / 16) - 0.625 * m for p, m in zip(product(mb_ref, mb_ref, k), upper(m_ref, k))]
            store(t_ref, k, t)
            mirror(tb_ref, k, t)
            mirror(vb_ref, k, [4.0 * x + 1.25 * m for x, m in zip(t, upper(m_ref, k))])
        for k in sides:
            mirror(ub_ref, k, [3.125 * t + p for t, p in zip(upper(t_ref, k), product(tb_ref, tb_ref, k))])
        for k in sides:
            y = [
                0.25 * p + (625 / 256) * t + (1.25 * 625 / 1024 - 0.3125) * m
                for p, t, m in zip(product(ub_ref, vb_ref, k), upper(t_ref, k), upper(m_ref, k))
            ]
            store(y_ref, k, y)
            mirror(tb_ref, k, y)
        for k in sides:
            t = [3.125 * y + p for y, p in zip(upper(y_ref, k), product(tb_ref, tb_ref, k))]
            store(t_ref, k, t)
            mirror(vb_ref, k, t)
        for k in sides:
            store(
                w_ref,
                k,
                [(625 / 128) * t + p for t, p in zip(upper(t_ref, k), product(vb_ref, vb_ref, k))],
            )
            add_diagonal(w_ref, k, jnp.full((1, 1), (625 / 256) ** 2 - CENTER, f32))
            mirror(ub_ref, k, upper(w_ref, k))
        for k in sides:
            t = [CENTER * m + p for m, p in zip(upper(m_ref, k), product(ub_ref, mb_ref, k))]
            store(t_ref, k, t)
            mirror(vb_ref, k, t)
        for k in sides:
            x = [
                (1.25 * y - (25 / 64) * t - 0.25 * p) * scales[k]
                for y, t, p in zip(upper(y_ref, k), upper(t_ref, k), product(tb_ref, vb_ref, k))
            ]
            store(m_ref, k, x)
            add_diagonal(m_ref, k, (125 / 64) * scales[k])
            mirror(mb_ref, k, upper(m_ref, k))

        tb_ref[0] = mm(mb_ref[0], g).astype(bf16)
        shaped = mm(tb_ref[0], mb_ref[1])
        m_ref[0] = shaped
        wide = g.astype(f32)
        entries = size * size
        top = jnp.sum(jnp.sum(wide * wide, axis=0, keepdims=True), axis=1, keepdims=True) / entries
        bottom = jnp.sum(jnp.sum(shaped * shaped, axis=0, keepdims=True), axis=1, keepdims=True) / entries
        scale = jnp.sqrt(top) / jnp.sqrt(bottom + epsilon)

        def rows_of(device):
            part = pl.ds(pl.multiple_of(device * stripe, stripe), stripe)
            return (m_ref[0, part, :] * scale).astype(bf16)

        if direct:
            for q in range(count):
                out_refs[q][...] = rows_of(lax.bitwise_xor(me, q))
        else:
            for r in range(chips):
                for c in range(2):
                    out_refs[r][c] = rows_of(lax.bitwise_xor(chip, r) * 2 + c)

    @pl.when(jnp.logical_not(active))
    def _():
        for k in sides:
            n_ref[k] = states[k][slot]
            stores[k].start()
        for out_ref in out_refs:
            out_ref[...] = jnp.zeros_like(out_ref)

    for k in sides:
        stores[k].wait()


def run_slot(slot, direct, scal, pieces, left, right, chain):
    size = left.shape[-1]
    stripe = pieces[0].shape[1]
    count = size // stripe
    wide = pltpu.VMEM((2, size, size), f32)
    narrow = pltpu.VMEM((2, size, size), bf16)
    sem = pltpu.SemaphoreType.DMA((2,))
    if direct:
        out = [(jax.ShapeDtypeStruct((stripe, size), bf16), VMEM)] * count
    else:
        out = [(jax.ShapeDtypeStruct((2, stripe, size), bf16), VMEM)] * (count // 2)
    news = [(jax.ShapeDtypeStruct(state.shape, f32), ANY) for state in (left, right)]
    operands = [(scal, SMEM), (left, VMEM), (right, VMEM)] + [(piece, VMEM) for piece in pieces]
    operands += [(state, ANY) for state in chain]
    aliases = {len(operands) - 2 + k: len(out) + k for k in range(2)} if chain else {}
    *updates, new_left, new_right = call(
        functools.partial(slot_kernel, slot, direct, count),
        out + news,
        [pltpu.VMEM((size, size), bf16)] + [wide] * 5 + [narrow] * 4 + [sem],
        operands,
        flops=40 * size**3,
        aliases=aliases,
        limit=LIMIT,
    )
    return updates, (new_left, new_right)


def tables(table_row, count):
    order = jnp.arange(count, dtype=jnp.int32)
    earlier = order[:, None] < order[None, :]
    matching = table_row[:, None] == table_row[None, :]
    rank = jnp.sum(jnp.logical_and(matching, earlier), axis=0).astype(jnp.int32)
    slots = jnp.arange(MOST, dtype=jnp.int32)
    chooser = jnp.logical_and(
        table_row[None, None, :] == order[None, :, None],
        rank[None, None, :] == slots[:, None, None],
    )
    block_of = jnp.sum(jnp.where(chooser, order, 0), axis=2).astype(jnp.int32)
    used = jnp.sum(chooser, axis=2).astype(jnp.int32)
    return jnp.concatenate([block_of.reshape(-1), used.reshape(-1)])


def step(grad_partial, owner_table, left_factor, right_factor):
    _, count, stripe, size = grad_partial.shape[1:]
    data_index = lax.axis_index("dp").astype(jnp.int32)
    owner_index = lax.axis_index("block").astype(jnp.int32)
    table_row = lax.dynamic_index_in_dim(owner_table, data_index, 0, keepdims=False)
    place_of = jnp.stack([data_index // 2, data_index % 2, owner_index])
    scal = jnp.concatenate([place_of, tables(table_row, count)])
    left, right = left_factor[0, 0], right_factor[0, 0]

    chips = count // 2
    cores = [(i, i ^ 1) for i in range(count)]
    total = sum_over_dp(grad_partial[0], place_of)
    other = lax.ppermute(total, "block", cores)
    message = (jax.ShapeDtypeStruct((2, stripe, size), bf16), VMEM)
    messages = call(
        functools.partial(arrange_kernel, count),
        [message] * (MOST * chips),
        [],
        [(scal, SMEM), (total, VMEM), (other, VMEM)],
    )
    pieces = []
    for slot in range(MOST):
        part = messages[slot * chips : (slot + 1) * chips]
        pieces.append(over_block(part, count, 2))

    states = [(state, VMEM) for state in (left, right)]
    kept = [(jax.ShapeDtypeStruct(left.shape, f32), VMEM)] * 2
    left, right = call(stage_kernel, kept, [], states)

    updates, chain = run_slot(0, False, scal, pieces[0], left, right, ())
    returned = over_block(updates, count, 2)
    updates, chain = run_slot(1, True, scal, pieces[1], left, right, chain)
    direct = over_block(updates, count, 1)
    (given,) = call(
        give_kernel,
        [(jax.ShapeDtypeStruct((chips, stripe, size), bf16), VMEM)],
        [],
        [(scal, SMEM)] + [(piece, VMEM) for piece in returned],
    )
    given = lax.ppermute(given, "block", cores)
    (placed,) = call(
        functools.partial(place_kernel, count),
        [(jax.ShapeDtypeStruct((count, stripe, size), bf16), VMEM)],
        [],
        [(scal, SMEM)] + [(piece, VMEM) for piece in returned + [given] + direct],
    )
    new_left, new_right = chain
    return placed[None], new_left[None, None], new_right[None, None]


def solution(mesh):
    placed = (
        P("dp", None, None, "block", None),
        P(),
        P("dp", "block", None, None, None),
        P("dp", "block", None, None, None),
    )
    return jax.shard_map(
        step,
        mesh=mesh,
        in_specs=placed,
        out_specs=(
            P("dp", None, "block", None),
            P("dp", "block", None, None, None),
            P("dp", "block", None, None, None),
        ),
        check_vma=False,
    )
```

```python
import functools

import jax
import jax.numpy as jnp
from jax import lax
from jax.experimental import pallas as pl
from jax.experimental.pallas import tpu as pltpu
from jax.sharding import PartitionSpec as P


MOST = 2
POWER = 8
CENTER = 3.6

decay_rate = 0.9
damping = 0.1
epsilon = 1e-06

f32 = jnp.float32
bf16 = jnp.bfloat16
SMEM = pltpu.SMEM
VMEM = pltpu.VMEM
ANY = pltpu.HBM
LIMIT = 24 * 1024 * 1024
SMALL = 8 * 1024 * 1024


def mm(a, b):
    return jnp.dot(a, b, preferred_element_type=f32)


def call(kernel, out_shape, scratch, operands, flops=0, aliases={}, limit=SMALL):
    outs = [shape for shape, _ in out_shape]
    size = sum(array.size * array.dtype.itemsize for array, _ in operands)
    return pl.pallas_call(
        kernel,
        in_specs=[pl.BlockSpec(memory_space=space) for _, space in operands],
        out_specs=[pl.BlockSpec(memory_space=space) for _, space in out_shape],
        out_shape=outs,
        scratch_shapes=scratch,
        input_output_aliases=aliases,
        compiler_params=pltpu.CompilerParams(vmem_limit_bytes=limit),
        cost_estimate=pl.CostEstimate(flops=flops, bytes_accessed=size, transcendentals=0),
    )(*[array for array, _ in operands])


def keep_kernel(scal, p_ref, a_ref, b_ref):
    cut = a_ref.shape[0]
    high, low = scal[0], scal[1]
    a_ref[...] = p_ref[1 - high, low, :cut]
    b_ref[...] = p_ref[high, 1 - low, cut:]


def forward_kernel(bit, scal, kept_ref, first_ref, out_ref):
    out_ref[...] = (kept_ref[...] + first_ref[1 - scal[bit]].astype(f32)).astype(bf16)


def half_kernel(scal, p_ref, *refs):
    *first_refs, own_ref = refs
    blocks = first_refs[0].shape[1]
    high, low = scal[0], scal[1]
    for index, ref in enumerate(first_refs):
        part = pl.ds(index * blocks, blocks)
        bit = 2 * index // len(first_refs)
        own_ref[part] = p_ref[high, low, part] + ref[(high, low)[bit]].astype(f32)


def total_kernel(own_ref, *refs):
    *second_refs, out_ref = refs
    blocks = second_refs[0].shape[0]
    for index, ref in enumerate(second_refs):
        part = pl.ds(index * blocks, blocks)
        out_ref[part] = (own_ref[part] + ref[...].astype(f32)).astype(bf16)


def sum_over_dp(grad_partial, scal):
    rows, count, stripe, size = grad_partial.shape
    p = grad_partial.reshape(2, rows // 2, count, stripe, size)
    over_low = [(i, i ^ 1) for i in range(rows)]
    over_high = [(i, i ^ 2) for i in range(rows)]
    cut = count // 2
    shape = (cut, stripe, size)
    one = (jax.ShapeDtypeStruct(shape, bf16), VMEM)
    both = (jax.ShapeDtypeStruct((count, stripe, size), bf16), VMEM)
    high, low = scal[0], scal[1]
    a = lax.dynamic_slice(p, (0, 1 - low, 0, 0, 0), (2, 1) + shape).reshape((2,) + shape)
    b = lax.dynamic_slice(p, (1 - high, 0, cut, 0, 0), (1, 2) + shape).reshape((2,) + shape)
    first = [
        lax.ppermute(a.astype(bf16), "dp", over_low),
        lax.ppermute(b.astype(bf16), "dp", over_high),
    ]
    fixed = [(scal, SMEM), (p, VMEM)]
    kept = [(jax.ShapeDtypeStruct(shape, f32), VMEM)] * 2
    kept = call(keep_kernel, kept, [], fixed)
    second = []
    for bit, perm in enumerate([over_high, over_low]):
        operands = [(scal, SMEM), (kept[bit], VMEM), (first[bit], VMEM)]
        kernel = functools.partial(forward_kernel, bit)
        (summed,) = call(kernel, [one], [], operands)
        second.append(lax.ppermute(summed, "dp", perm))
    whole = [(jax.ShapeDtypeStruct((count, stripe, size), f32), VMEM)]
    arrived = [(array, VMEM) for array in first]
    (own,) = call(half_kernel, whole, [], fixed + arrived)
    operands = [(own, VMEM)] + [(array, VMEM) for array in second]
    (total,) = call(total_kernel, [both], [], operands)
    return total


def arrange_kernel(count, scal, own_ref, other_ref, *out_refs):
    me = scal[2]
    core, chip = me % 2, me // 2
    chips = count // 2
    for slot in range(MOST):
        for r in range(chips):
            j = scal[3 + slot * count + lax.bitwise_xor(chip, r) * 2 + core]
            out_ref = out_refs[slot * chips + r]
            out_ref[core] = own_ref[j]
            out_ref[1 - core] = other_ref[j]


def stage_kernel(l_ref, r_ref, l_out, r_out):
    l_out[...] = l_ref[...]
    r_out[...] = r_ref[...]


def give_kernel(scal, *refs):
    *in_refs, out_ref = refs
    core = scal[2] % 2
    for r, in_ref in enumerate(in_refs):
        out_ref[r] = in_ref[1 - core]


def place_kernel(count, scal, *refs):
    *in_refs, out_ref = refs
    me = scal[2]
    core, chip = me % 2, me // 2
    chips = count // 2
    pieces = []
    for r in range(chips):
        base = lax.bitwise_xor(chip, r) * 2
        pieces.append((base + core, in_refs[r], core))
        pieces.append((base + 1 - core, in_refs[chips], r))
    for q in range(count):
        pieces.append((count + lax.bitwise_xor(me, q), in_refs[chips + 1 + q], None))
    for entry, ref, index in pieces:
        at = 3 + entry

        @pl.when(scal[at + MOST * count] > 0)
        def _(at=at, ref=ref, index=index):
            out_ref[scal[at]] = ref[...] if index is None else ref[index]


def over_block(arrays, count, stride):
    moved = [arrays[0]]
    for r in range(1, len(arrays)):
        pairs = [(i, i ^ (r * stride)) for i in range(count)]
        moved.append(lax.ppermute(arrays[r], "block", pairs))
    return moved


def add_diagonal(ref, k, value):
    size = ref.shape[1]
    width = min(size, 128)
    rows = lax.broadcasted_iota(jnp.int32, (width, width), 0)
    columns = lax.broadcasted_iota(jnp.int32, (width, width), 1)
    spread = jnp.where(rows == columns, value, 0.0)
    for start in range(0, size, width):
        part = pl.ds(start, width)
        ref[k, part, part] += spread


def times_row(ref, k, row):
    size = ref.shape[1]
    step = min(size, 64)
    return jnp.concatenate(
        [
            jnp.sum(ref[k, pl.ds(start, step), :] * row, axis=1, keepdims=True)
            for start in range(0, size, step)
        ]
    )


def times_column(ref, k, column):
    total = 0.0
    for start in range(0, ref.shape[1], 8):
        total += ref[k, pl.ds(start, 8), :] * column[start : start + 8]
    return jnp.sum(total, axis=0, keepdims=True)


def product(a_ref, b_ref, k):
    half = a_ref.shape[1] // 2
    return mm(a_ref[k, :half, :], b_ref[k]), mm(a_ref[k, half:, :], b_ref[k, :, half:])


def upper(ref, k):
    half = ref.shape[1] // 2
    return ref[k, :half, :], ref[k, half:, half:]


def store(ref, k, blocks):
    half = ref.shape[1] // 2
    ref[k, :half, :] = blocks[0]
    ref[k, half:, half:] = blocks[1]


def mirror(ref, k, blocks):
    half = ref.shape[1] // 2
    top = blocks[0].astype(bf16)
    ref[k, :half, :] = top
    ref[k, half:, half:] = blocks[1].astype(bf16)
    ref[k, half:, :half] = top[:, half:].T


def slot_kernel(slot, direct, count, scal, l_ref, r_ref, *refs):
    chips = count // 2
    in_refs, refs = refs[:chips], refs[chips + (2 if slot else 0) :]
    n_out = count if direct else chips
    out_refs, refs = refs[:n_out], refs[n_out:]
    lo_hbm, ro_hbm, g_ref, n_ref, m_ref, t_ref, y_ref, w_ref = refs[:8]
    mb_ref, tb_ref, ub_ref, vb_ref, out_sem = refs[8:]
    size = g_ref.shape[0]
    stripe = size // count
    me = scal[2]
    chip = me // 2
    sides = (0, 1)
    states = (l_ref, r_ref)
    news = (lo_hbm, ro_hbm)
    stores = [pltpu.make_async_copy(n_ref.at[k], news[k].at[slot], out_sem.at[k]) for k in sides]
    active = scal[3 + (MOST + slot) * count + me] > 0

    @pl.when(active)
    def _():
        for r, ref in enumerate(in_refs):
            for c in range(2):
                start = pl.multiple_of((lax.bitwise_xor(chip, r) * 2 + c) * stripe, stripe)
                g_ref[pl.ds(start, stripe), :] = ref[c]
        g = g_ref[...]
        contract = ((1,), (0,))
        for k in sides:
            dims = ((contract[k], contract[k]), ((), ()))
            term = lax.dot_general(g, g, dims, preferred_element_type=f32)
            new = decay_rate * states[k][slot] + term * ((1.0 - decay_rate) / size)
            n_ref[k] = new
            m_ref[k] = new
            stores[k].start()
        for k in sides:
            add_diagonal(m_ref, k, jnp.full((1, 1), damping, f32))

        vectors = [jnp.full((1, size), size**-0.5, f32)] * 2
        lengths = [None, None]
        for turn in range(POWER):
            for k in sides:
                vectors[k] = (times_column if turn % 2 else times_row)(m_ref, k, vectors[k])
            for k in sides:
                square = jnp.sum(vectors[k] * vectors[k], axis=turn % 2, keepdims=True)
                lengths[k] = jnp.sqrt(square)
                vectors[k] = vectors[k] / lengths[k]

        scales = []
        for k in sides:
            ceiling = 1.25 * lengths[k]
            scales.append(lax.rsqrt(jnp.sqrt(ceiling)))
            scaled = m_ref[k] * (1.0 / ceiling)
            m_ref[k] = scaled
            mb_ref[k] = scaled.astype(bf16)
        for k in sides:
            t = [p * (1 / 16) - 0.625 * m for p, m in zip(product(mb_ref, mb_ref, k), upper(m_ref, k))]
            store(t_ref, k, t)
            mirror(tb_ref, k, t)
            mirror(vb_ref, k, [4.0 * x + 1.25 * m for x, m in zip(t, upper(m_ref, k))])
        for k in sides:
            mirror(ub_ref, k, [3.125 * t + p for t, p in zip(upper(t_ref, k), product(tb_ref, tb_ref, k))])
        for k in sides:
            y = [
                0.25 * p + (625 / 256) * t + (1.25 * 625 / 1024 - 0.3125) * m
                for p, t, m in zip(product(ub_ref, vb_ref, k), upper(t_ref, k), upper(m_ref, k))
            ]
            store(y_ref, k, y)
            mirror(tb_ref, k, y)
        for k in sides:
            t = [3.125 * y + p for y, p in zip(upper(y_ref, k), product(tb_ref, tb_ref, k))]
            store(t_ref, k, t)
            mirror(vb_ref, k, t)
        for k in sides:
            store(
                w_ref,
                k,
                [(625 / 128) * t + p for t, p in zip(upper(t_ref, k), product(vb_ref, vb_ref, k))],
            )
            add_diagonal(w_ref, k, jnp.full((1, 1), (625 / 256) ** 2 - CENTER, f32))
            mirror(ub_ref, k, upper(w_ref, k))
        for k in sides:
            t = [CENTER * m + p for m, p in zip(upper(m_ref, k), product(ub_ref, mb_ref, k))]
            store(t_ref, k, t)
            mirror(vb_ref, k, t)
        for k in sides:
            x = [
                (1.25 * y - (25 / 64) * t - 0.25 * p) * scales[k]
                for y, t, p in zip(upper(y_ref, k), upper(t_ref, k), product(tb_ref, vb_ref, k))
            ]
            store(m_ref, k, x)
            add_diagonal(m_ref, k, (125 / 64) * scales[k])
            mirror(mb_ref, k, upper(m_ref, k))

        tb_ref[0] = mm(mb_ref[0], g).astype(bf16)
        shaped = mm(tb_ref[0], mb_ref[1])
        m_ref[0] = shaped
        wide = g.astype(f32)
        entries = size * size
        top = jnp.sum(jnp.sum(wide * wide, axis=0, keepdims=True), axis=1, keepdims=True) / entries
        bottom = jnp.sum(jnp.sum(shaped * shaped, axis=0, keepdims=True), axis=1, keepdims=True) / entries
        scale = jnp.sqrt(top) / jnp.sqrt(bottom + epsilon)

        def rows_of(device):
            part = pl.ds(pl.multiple_of(device * stripe, stripe), stripe)
            return (m_ref[0, part, :] * scale).astype(bf16)

        if direct:
            for q in range(count):
                out_refs[q][...] = rows_of(lax.bitwise_xor(me, q))
        else:
            for r in range(chips):
                for c in range(2):
                    out_refs[r][c] = rows_of(lax.bitwise_xor(chip, r) * 2 + c)

    @pl.when(jnp.logical_not(active))
    def _():
        for k in sides:
            n_ref[k] = states[k][slot]
            stores[k].start()
        for out_ref in out_refs:
            out_ref[...] = jnp.zeros_like(out_ref)

    for k in sides:
        stores[k].wait()


def run_slot(slot, direct, scal, pieces, left, right, chain):
    size = left.shape[-1]
    stripe = pieces[0].shape[1]
    count = size // stripe
    wide = pltpu.VMEM((2, size, size), f32)
    narrow = pltpu.VMEM((2, size, size), bf16)
    sem = pltpu.SemaphoreType.DMA((2,))
    if direct:
        out = [(jax.ShapeDtypeStruct((stripe, size), bf16), VMEM)] * count
    else:
        out = [(jax.ShapeDtypeStruct((2, stripe, size), bf16), VMEM)] * (count // 2)
    news = [(jax.ShapeDtypeStruct(state.shape, f32), ANY) for state in (left, right)]
    operands = [(scal, SMEM), (left, VMEM), (right, VMEM)] + [(piece, VMEM) for piece in pieces]
    operands += [(state, ANY) for state in chain]
    aliases = {len(operands) - 2 + k: len(out) + k for k in range(2)} if chain else {}
    *updates, new_left, new_right = call(
        functools.partial(slot_kernel, slot, direct, count),
        out + news,
        [pltpu.VMEM((size, size), bf16)] + [wide] * 5 + [narrow] * 4 + [sem],
        operands,
        flops=40 * size**3,
        aliases=aliases,
        limit=LIMIT,
    )
    return updates, (new_left, new_right)


def tables(table_row, count):
    order = jnp.arange(count, dtype=jnp.int32)
    earlier = order[:, None] < order[None, :]
    matching = table_row[:, None] == table_row[None, :]
    rank = jnp.sum(jnp.logical_and(matching, earlier), axis=0).astype(jnp.int32)
    slots = jnp.arange(MOST, dtype=jnp.int32)
    chooser = jnp.logical_and(
        table_row[None, None, :] == order[None, :, None],
        rank[None, None, :] == slots[:, None, None],
    )
    block_of = jnp.sum(jnp.where(chooser, order, 0), axis=2).astype(jnp.int32)
    used = jnp.sum(chooser, axis=2).astype(jnp.int32)
    return jnp.concatenate([block_of.reshape(-1), used.reshape(-1)])


def step(grad_partial, owner_table, left_factor, right_factor):
    _, count, stripe, size = grad_partial.shape[1:]
    data_index = lax.axis_index("dp").astype(jnp.int32)
    owner_index = lax.axis_index("block").astype(jnp.int32)
    table_row = lax.dynamic_index_in_dim(owner_table, data_index, 0, keepdims=False)
    place_of = jnp.stack([data_index // 2, data_index % 2, owner_index])
    scal = jnp.concatenate([place_of, tables(table_row, count)])
    left, right = left_factor[0, 0], right_factor[0, 0]

    chips = count // 2
    cores = [(i, i ^ 1) for i in range(count)]
    total = sum_over_dp(grad_partial[0], place_of)
    other = lax.ppermute(total, "block", cores)
    message = (jax.ShapeDtypeStruct((2, stripe, size), bf16), VMEM)
    messages = call(
        functools.partial(arrange_kernel, count),
        [message] * (MOST * chips),
        [],
        [(scal, SMEM), (total, VMEM), (other, VMEM)],
    )
    pieces = []
    for slot in range(MOST):
        part = messages[slot * chips : (slot + 1) * chips]
        pieces.append(over_block(part, count, 2))

    states = [(state, VMEM) for state in (left, right)]
    kept = [(jax.ShapeDtypeStruct(left.shape, f32), VMEM)] * 2
    left, right = call(stage_kernel, kept, [], states)

    updates, chain = run_slot(0, False, scal, pieces[0], left, right, ())
    returned = over_block(updates, count, 2)
    updates, chain = run_slot(1, True, scal, pieces[1], left, right, chain)
    direct = over_block(updates, count, 1)
    (given,) = call(
        give_kernel,
        [(jax.ShapeDtypeStruct((chips, stripe, size), bf16), VMEM)],
        [],
        [(scal, SMEM)] + [(piece, VMEM) for piece in returned],
    )
    given = lax.ppermute(given, "block", cores)
    (placed,) = call(
        functools.partial(place_kernel, count),
        [(jax.ShapeDtypeStruct((count, stripe, size), bf16), VMEM)],
        [],
        [(scal, SMEM)] + [(piece, VMEM) for piece in returned + [given] + direct],
    )
    new_left, new_right = chain
    return placed[None], new_left[None, None], new_right[None, None]


def solution(mesh):
    placed = (
        P("dp", None, None, "block", None),
        P(),
        P("dp", "block", None, None, None),
        P("dp", "block", None, None, None),
    )
    return jax.shard_map(
        step,
        mesh=mesh,
        in_specs=placed,
        out_specs=(
            P("dp", None, "block", None),
            P("dp", "block", None, None, None),
            P("dp", "block", None, None, None),
        ),
        check_vma=False,
    )
```
